32 devices in a mesh: rows: 16 (over z, x, core), cols: 2 (over y).
Axes of the slice: x: 2, y: 2, z: 4, core: 2. Of those that a mesh axis runs over, the one named last changes fastest.
Arguments:
- image: float32 [1024, 16384], P('rows', 'cols'), may hold values from -6 to 6
- cloud_mask: int32 [1024, 16384], P('rows', 'cols'), may hold values 0 or 1
- tile_weight: int32 [128, 128], P('rows', 'cols'), may hold values from 1 to 8
- owner: int32 [128], replicated, may hold values from 0 to 15, as said below
Outputs:
- solution: float32 [1024, 16384], P('rows', 'cols')
- objective: float32 [3], replicated
The draws below stay inside these ranges and needn't reach their ends.
Inputs may be any that keep to these rules, and one draw needn't show every extreme that they name: `owner`: every index of rows owns exactly 8 blocks, and the 8 blocks b*8 to b*8 + 7 have 8 different owners for every b.
All inputs are finite; a program needn't handle non-finite values. No bound on the sum of `cloud_mask` on one device may be relied on, other than what follows from the above.
Results may differ from the reference program's by a relative error of at most 0.0001.
Values sent between devices are 32-bit elements; how exact they have to be, the bound alone decides.
A program may use at most 64 MiB of HBM per device.

```python
import jax
import jax.numpy as jnp

BR = 8
BPD = 8
W = 16384
TW = 128
ITERS = 3
NBLK = 128
H = 1024
N_ROWS = 16


def draw_owner(key, part):
    folded = jax.random.fold_in(key, 11)
    shuffled = jax.random.permutation(jax.random.fold_in(folded, 1), N_ROWS).astype(jnp.int32)
    ranks = jnp.argsort(shuffled).astype(jnp.int32)
    values = jnp.arange(N_ROWS, dtype=jnp.int32)
    special = ((values == 1) | (values == N_ROWS // 2)).astype(jnp.int32)
    scores = ranks - 2 * N_ROWS * special
    offsets = jnp.argsort(scores).astype(jnp.int32)[:BPD]
    subkeys = jax.random.split(jax.random.fold_in(folded, 2), N_ROWS)
    orders = jax.vmap(lambda sub_key: jax.random.permutation(sub_key, BPD))(subkeys)
    source = jnp.arange(N_ROWS, dtype=jnp.int32)[:, None]
    owners = (source + offsets[orders]) % N_ROWS
    return owners.reshape(-1).astype(jnp.int32)


def set_ends(values, rng, smallest, largest):
    place = [jax.random.randint(jax.random.fold_in(rng, axis), (), 0, length) for axis, length in enumerate(values.shape)]
    longest = values.shape.index(max(values.shape))
    neighbour = place[:longest] + [(place[longest] + 1) % values.shape[longest]] + place[longest + 1:]
    return values.at[tuple(place)].set(smallest).at[tuple(neighbour)].set(largest)


def block_scale(key, extent, pieces, smallest, largest):
    gain = 1.0
    for axis_at, blocks in pieces:
        draws = jax.random.uniform(jax.random.fold_in(jax.random.fold_in(key, 6), axis_at), (blocks,), jnp.float32, smallest / len(pieces), largest / len(pieces))
        gain = gain * jnp.repeat(jnp.exp(draws), extent[axis_at] // blocks).reshape((-1,) + (1,) * (len(extent) - 1 - axis_at))
    return gain


def noise(own_key, dims, deviation, limit, cuts=(), kind=jnp.bfloat16):
    result = deviation * jax.random.normal(own_key, dims, jnp.float32)
    if cuts:
        result = result * block_scale(own_key, dims, cuts, -0.22, 0.18)
    return jnp.clip(result, -limit, limit).astype(kind)


def setup_inputs(seed: int = 0) -> dict:
    key_of = jax.random.split(jax.random.key(seed), 5)
    return {
        "image": noise(key_of[0], (H, W), 1.0, 6.0, ((0, 16), (1, 2)), jnp.float32),
        "cloud_mask": set_ends((jax.random.randint(key_of[1], (H, W), 0, 3) < 1).astype(jnp.int32), jax.random.fold_in(key_of[1], 1), 0, 1),
        "tile_weight": set_ends(jax.random.randint(key_of[2], (NBLK, W // TW), 1, 9), jax.random.fold_in(key_of[2], 1), 1, 8).astype(jnp.int32),
        "owner": draw_owner(jax.random.fold_in(key_of[4], 71), 0),
    }


fidelity_scale = 0.25
tau_step = 0.35
sigma_step = 0.35
tv_weight = 0.3

def forward_rows(field):
    return jnp.concatenate([field[1:] - field[:-1], jnp.zeros_like(field[:1])], axis=0)

def forward_cols(field):
    return jnp.concatenate([field[:, 1:] - field[:, :-1], jnp.zeros_like(field[:, :1])], axis=1)

def divergence(dual_rows, dual_cols):
    above = jnp.concatenate([jnp.zeros_like(dual_rows[:1]), dual_rows[:-1]], axis=0)
    leftward = jnp.concatenate([jnp.zeros_like(dual_cols[:, :1]), dual_cols[:, :-1]], axis=1)
    return dual_rows - above + (dual_cols - leftward)

def reference(image, cloud_mask, tile_weight, owner):
    height, width = image.shape
    total_blocks = owner.shape[0]
    tile_count = tile_weight.shape[1]
    per_tile = jnp.broadcast_to(tile_weight.astype(jnp.float32)[:, None, :, None], (total_blocks, BR, tile_count, TW)).reshape(height, width)
    fidelity = fidelity_scale * per_tile * (1 - cloud_mask).astype(jnp.float32)
    primal = image
    extrap = image
    dual_rows = jnp.zeros_like(image)
    dual_cols = jnp.zeros_like(image)
    objective_list = []
    for step in range(ITERS):
        grad_r = forward_rows(extrap)
        grad_c = forward_cols(extrap)
        trial_rows = dual_rows + sigma_step * grad_r
        trial_cols = dual_cols + sigma_step * grad_c
        shrink = jnp.maximum(1.0, jnp.sqrt(trial_rows * trial_rows + trial_cols * trial_cols) / tv_weight)
        dual_rows = trial_rows / shrink
        dual_cols = trial_cols / shrink
        updated = (primal + tau_step * divergence(dual_rows, dual_cols) + tau_step * fidelity * image) / (1.0 + tau_step * fidelity)
        misfit = updated - image
        total = jnp.sum(0.5 * fidelity * misfit * misfit) + tv_weight * jnp.sum(jnp.sqrt(grad_r * grad_r + grad_c * grad_c))
        objective_list.append(total / (height * width))
        extrap = 2.0 * updated - primal
        primal = updated
    order = jnp.argsort(owner, stable=True)
    solution = primal.reshape(total_blocks, BR, width)[order].reshape(height, width)
    return (solution, jnp.stack(objective_list).astype(jnp.float32))
```

```python
import functools

import jax
import jax.numpy as jnp
from jax import lax
from jax.experimental import pallas as pl
from jax.experimental.pallas import tpu as pltpu
from jax.sharding import PartitionSpec as P

MESH = pl.DeviceIdType.MESH
BR = 8
TW = 128
ITERS = 3
GROUP = 8
LAG = 16
RING = 8
TINY = 1.2e-38

fidelity_scale = 0.25
tau_step = 0.35
sigma_step = 0.35
tv_weight = 0.3


def kernel(
    n_rows,
    n_cols,
    pixel_total,
    runs,
    weight_ref,
    owner_ref,
    image_ref,
    mask_ref,
    out_ref,
    obj_ref,
    field,
    fid,
    mask,
    pr0,
    pr1,
    pr2,
    pc0,
    pc1,
    pc2,
    er0,
    er1,
    er2,
    cr0,
    cr1,
    cr2,
    e0,
    e1,
    ex0,
    ex1,
    done,
    outbox,
    inbox,
    outv,
    pick,
    sender,
    part,
    part_in,
    total,
    total_in,
    load_sem,
    mask_sem,
    out_sem,
    halo_send,
    halo_recv,
    side_send,
    side_recv,
    a2a_send,
    a2a_recv,
    part_send,
    part_recv,
    total_send,
    total_recv,
):
    rows_here, width = image_ref.shape
    blocks = rows_here // BR
    tiles = width // TW
    group = min(GROUP, tiles)
    strips = tiles // group
    ext_blocks = blocks + 2
    ext_rows = rows_here + 2 * BR
    ext_tiles = tiles + 2
    me = lax.axis_index("rows")
    my_col = lax.axis_index("cols")
    has_up, has_down = me > 0, me < n_rows - 1
    has_left, has_right = my_col > 0, my_col < n_cols - 1
    own = pl.ds(BR, rows_here)

    def load_image(c, i):
        t = c * group + i
        return pltpu.make_async_copy(
            image_ref.at[:, pl.ds(pl.multiple_of(t * TW, TW), TW)],
            field.at[0, LAG + 1 + t, own],
            load_sem.at[c],
        )

    def load_mask(c):
        cols = pl.ds(pl.multiple_of(c * group * TW, TW), group * TW)
        return pltpu.make_async_copy(mask_ref.at[:, cols], mask.at[:, cols], mask_sem.at[c])

    @pl.loop(0, strips)
    def _(c):
        load_mask(c).start()

        @pl.loop(0, group)
        def _(i):
            load_image(c, i).start()

    barrier = pltpu.get_barrier_semaphore()

    @pl.loop(1, n_rows)
    def _(k):
        pl.semaphore_signal(
            barrier, inc=1, device_id={"rows": lax.rem(me + k, n_rows)}, device_id_type=MESH
        )

    @pl.loop(1, n_cols)
    def _(k):
        pl.semaphore_signal(
            barrier, inc=1, device_id={"cols": lax.rem(my_col + k, n_cols)}, device_id_type=MESH
        )

    up_row, down_row = lax.rem(me + n_rows - 1, n_rows), lax.rem(me + 1, n_rows)
    left_col, right_col = lax.rem(my_col + n_cols - 1, n_cols), lax.rem(my_col + 1, n_cols)
    for r in (up_row, down_row):
        for c in (left_col, right_col):
            pl.semaphore_signal(
                barrier, inc=1, device_id={"rows": r, "cols": c}, device_id_type=MESH
            )

    @pl.loop(0, n_rows)
    def _(d):
        found = jnp.int32(0)
        for b in range(blocks):
            found = jnp.where(owner_ref[me * blocks + b] == d, b, found)
        pick[d] = found

    def find_sender(s, carry):
        count, slots = carry
        mine = jnp.int32(0)
        for b in range(blocks):
            mine = jnp.where(owner_ref[s * blocks + b] == me, 1, mine)
        slots = [jnp.where((mine == 1) & (count == j), s, slots[j]) for j in range(blocks)]
        return count + mine, slots

    _, slots = lax.fori_loop(
        0, n_rows, find_sender, (jnp.int32(0), [jnp.int32(0)] * blocks)
    )
    for j in range(blocks):
        sender[j] = slots[j]

    @pl.loop(0, strips)
    def _(c):
        load_mask(c).wait()
        inner = field.at[0, pl.ds(LAG + 1 + c * group, group), own]
        pltpu.make_async_copy(inner, inner, load_sem.at[c]).wait()

        @pl.loop(0, group)
        def _(i):
            t = c * group + i
            col = pl.ds(pl.multiple_of(t * TW, TW), TW)
            for b in range(blocks):
                clear = (1 - mask[b * BR : (b + 1) * BR, col]).astype(jnp.float32)
                f = (fidelity_scale * weight_ref[b, t].astype(jnp.float32)) * clear
                fid[LAG + 1 + t, b * BR : (b + 1) * BR] = f
                field[1, LAG + 1 + t, (b + 1) * BR : (b + 2) * BR] = 1.0 / (1.0 + tau_step * f)

    zero = jnp.zeros((BR, TW), jnp.float32)
    slopes_r, slopes_c = (pr0, pr1, pr2), (pc0, pc1, pc2)
    rolled_e, rolled_c = (er0, er1, er2), (cr0, cr1, cr2)
    for pc in slopes_c:
        for b in range(ext_blocks):
            pc[RING, b * BR : (b + 1) * BR] = zero

    pl.semaphore_wait(barrier, n_rows - 1 + n_cols - 1 + 4)

    top, bottom = pl.ds(BR, BR), pl.ds(rows_here, BR)
    above, below_rows = pl.ds(0, BR), pl.ds(ext_rows - BR, BR)

    def halo(way, c):
        cols = pl.ds(LAG + 1 + c * group, group)
        src, dst = ((top, below_rows), (bottom, above))[way]
        return pltpu.make_async_remote_copy(
            src_ref=field.at[:, cols, src],
            dst_ref=field.at[:, cols, dst],
            send_sem=halo_send.at[way],
            recv_sem=halo_recv.at[way, c],
            device_id={"rows": (up_row, down_row)[way]},
            device_id_type=MESH,
        )

    def side(way, piece):
        src_col, dst_col = ((1, ext_tiles - 1), (ext_tiles - 2, 0))[way]
        src, dst = ((own, own), (top, below_rows), (bottom, above))[piece]
        device = {"cols": (left_col, right_col)[way]}
        if piece:
            device["rows"] = (up_row, down_row)[piece - 1]
        return pltpu.make_async_remote_copy(
            src_ref=field.at[:, pl.ds(LAG + src_col, 1), src],
            dst_ref=field.at[:, pl.ds(LAG + dst_col, 1), dst],
            send_sem=side_send.at[way, piece],
            recv_sem=side_recv.at[way, piece],
            device_id=device,
            device_id_type=MESH,
        )

    has_side, has_row = (has_left, has_right), (has_up, has_down)

    def on_sides(way, act):
        @pl.when(has_side[way])
        def _():
            act(side(way, 0))
            for piece in (1, 2):

                @pl.when(has_row[piece - 1])
                def _():
                    act(side(way, piece))

    def wait_side(way):
        @pl.when(has_side[1 - way])
        def _():
            side(way, 0).wait_recv()

            @pl.when(has_down)
            def _():
                side(way, 1).wait_recv()

            @pl.when(has_up)
            def _():
                side(way, 2).wait_recv()

    def on_rows(c, act_up, act_down):
        @pl.when(has_up)
        def _():
            act_up(c)

        @pl.when(has_down)
        def _():
            act_down(c)

    on_sides(1, lambda copy: copy.start())

    @pl.loop(0, strips)
    def _(c):
        on_rows(c, lambda c: halo(0, c).start(), lambda c: halo(1, c).start())

    on_sides(0, lambda copy: copy.start())

    def wait_halo(c):
        on_rows(c, lambda c: halo(1, c).wait_recv(), lambda c: halo(0, c).wait_recv())

    wait_side(1)

    sub = lax.broadcasted_iota(jnp.int32, (BR, TW), 0)
    lane = lax.broadcasted_iota(jnp.int32, (BR, TW), 1)
    first_lane, last_lane = lane == 0, lane == TW - 1
    end_row = jnp.logical_and(sub == BR - 1, jnp.logical_not(has_down))
    end_col = jnp.logical_and(last_lane, jnp.logical_not(has_right))
    reach = tv_weight / sigma_step
    gain_step = tau_step * sigma_step
    def blk(b):
        return slice(b * BR, (b + 1) * BR)

    def slot(at):
        return lax.rem(at + 2 * RING, RING)

    def ahead(step, at, rows):
        return field[0, LAG + at, rows] if step == 0 else (ex0, ex1)[step - 1][slot(at), rows]

    def inside(at, acc):
        return jnp.where(jnp.logical_and(at >= 1, at <= tiles), acc, 0.0)

    def roll_ahead(step, at):
        into = rolled_e[step]
        for b in range(ext_blocks if step < ITERS - 1 else ext_blocks - 1):
            e, after = ahead(step, at, blk(b)), ahead(step, at + 1, blk(b))
            into[slot(at), blk(b)] = pltpu.roll(jnp.where(first_lane, after, e), TW - 1, 1)

    def roll_slope(step, at):
        into, pc = rolled_c[step], slopes_c[step]
        edge = jnp.logical_and(at == 1, jnp.logical_not(has_left))
        before = jnp.where(edge, RING, slot(at - 1))
        for b in range(ext_blocks) if step < ITERS - 1 else range(1, blocks + 1):
            prior, here = pc[before, blk(b)], pc[slot(at), blk(b)]
            into[slot(at), blk(b)] = pltpu.roll(jnp.where(last_lane, prior, here), 1, 1)

    def dual(step, at):
        t = slot(at)
        stop_here = jnp.logical_and(end_col, at == tiles)
        pr, pc = slopes_r[step], slopes_c[step]
        acc = zero
        for b in range(ext_blocks if step < ITERS - 1 else ext_blocks - 1):
            e = ahead(step, at, blk(b))
            if b < ext_blocks - 1:
                below = ahead(step, at, slice(b * BR + 1, (b + 1) * BR + 1))
            else:
                below = pltpu.roll(e, BR - 1, 0)
            g_r = below - e
            if b == blocks:
                g_r = jnp.where(end_row, 0.0, g_r)
            g_c = jnp.where(stop_here, 0.0, rolled_e[step][t, blk(b)] - e)
            mine = 0 < b <= blocks
            if step == 0:
                q_r, q_c = g_r, g_c
                q2 = q_r * q_r + q_c * q_c
                inv_len = lax.rsqrt(jnp.maximum(q2, TINY))
                if mine:
                    acc = acc + q2 * inv_len
            else:
                q_r = g_r + slopes_r[step - 1][t, blk(b)]
                q_c = g_c + slopes_c[step - 1][t, blk(b)]
                inv_len = lax.rsqrt(q_r * q_r + q_c * q_c)
                if mine:
                    g2 = g_r * g_r + g_c * g_c
                    acc = acc + g2 * lax.rsqrt(jnp.maximum(g2, TINY))
            inv = jnp.minimum(1.0, reach * inv_len)
            p_r = q_r * inv
            if b == 0:
                p_r = jnp.where(has_up, p_r, 0.0)
            pr[t, blk(b)] = p_r
            pc[t, blk(b)] = q_c * inv
        return inside(at, acc)

    def primal(step, at):
        t, full = slot(at), LAG + at
        pr, pc = slopes_r[step], slopes_c[step]
        acc = zero
        for b in range(ext_blocks) if step < ITERS - 1 else range(1, blocks + 1):
            p_r, p_c = pr[t, blk(b)], pc[t, blk(b)]
            if b > 0:
                over = pr[t, b * BR - 1 : (b + 1) * BR - 1]
            else:
                over = pltpu.roll(p_r, 1, 0)
            div = gain_step * ((p_r - over) + (p_c - rolled_c[step][t, blk(b)]))
            observed, g = field[0, full, blk(b)], field[1, full, blk(b)]
            if step == 0:
                e = div * g
                e0[t, blk(b)] = e
                ex0[t, blk(b)] = observed + 2.0 * e
            elif step == 1:
                old = e0[t, blk(b)]
                e = (old + div) * g
                e1[t, blk(b)] = e
                ex1[t, blk(b)] = (observed - old) + 2.0 * e
            else:
                e = (e1[t, blk(b)] + div) * g
                done[full, b - 1] = observed + e
            if 0 < b <= blocks:
                acc = acc + fid[full, blk(b - 1)] * (e * e)
        return inside(at, acc)

    def sweep(t, sums):
        sums = list(sums)
        for step in reversed(range(ITERS)):
            at = t - 5 * step
            sums[2 * step] += primal(step, at - 3)
            roll_slope(step, at - 2)
            sums[2 * step + 1] += dual(step, at - 1)
            roll_ahead(step, at)
        return tuple(sums)

    def block_copy(k, j):
        target = lax.rem(me + k, n_rows)
        part_of = pl.ds(j * group, group)
        return pltpu.make_async_remote_copy(
            src_ref=outbox.at[target, part_of],
            dst_ref=inbox.at[me, part_of],
            send_sem=a2a_send,
            recv_sem=a2a_recv,
            device_id={"rows": target},
            device_id_type=MESH,
        )

    def strip(j, sums):
        @pl.when(j < strips)
        def _():
            wait_halo(j)

        @pl.when(j == strips)
        def _():
            wait_side(0)

        sums = lax.fori_loop(0, group, lambda i, s: sweep(j * group + i - 2, s), sums)

        @pl.when(j > 1)
        def _():
            here = pl.ds((j - 2) * group, group)
            ext_here = pl.ds(LAG + 1 + (j - 2) * group, group)
            for first, stop in runs:

                @pl.loop(first, stop)
                def _(k):
                    target = lax.rem(me + k, n_rows)
                    outbox[target, here] = done[ext_here, pick[target]]
                    block_copy(k, j - 2).start()

            inbox[me, here] = done[ext_here, pick[me]]

        return sums

    sums = lax.fori_loop(0, strips + 2, strip, (zero,) * (2 * ITERS))

    stacked = zero
    for step in range(ITERS):
        acc = 0.5 * sums[2 * step] + tv_weight * sums[2 * step + 1]
        one = jnp.sum(jnp.sum(acc, axis=1, keepdims=True), axis=0, keepdims=True)
        stacked = jnp.where(sub == step, one, stacked)
    part[...] = stacked

    def part_copy(k):
        return pltpu.make_async_remote_copy(
            src_ref=part,
            dst_ref=part_in.at[me],
            send_sem=part_send,
            recv_sem=part_recv,
            device_id={"rows": lax.rem(me + k, n_rows)},
            device_id_type=MESH,
        )

    def all_of(buffer, count, sem):
        some = buffer.at[pl.ds(0, count)]
        pltpu.make_async_copy(some, some, sem).wait()

    @pl.loop(1, n_rows)
    def _(k):
        part_copy(k).start()

    part_in[me] = stacked

    all_of(part_in, n_rows - 1, part_recv)

    total_here = lax.fori_loop(0, n_rows, lambda k, s: s + part_in[k], zero)
    total[...] = total_here
    total_in[my_col] = total_here

    def total_copy(k):
        return pltpu.make_async_remote_copy(
            src_ref=total,
            dst_ref=total_in.at[my_col],
            send_sem=total_send,
            recv_sem=total_recv,
            device_id={"cols": lax.rem(my_col + k, n_cols)},
            device_id_type=MESH,
        )

    @pl.loop(1, n_cols)
    def _(k):
        total_copy(k).start()

    all_of(total_in, n_cols - 1, total_recv)

    everything = lax.fori_loop(0, n_cols, lambda k, s: s + total_in[k], zero)
    everything = everything / pixel_total
    for step in range(ITERS):
        obj_ref[step] = everything[step, 0]

    sent = sum(stop - first for first, stop in runs)
    all_of(inbox, sent, a2a_recv)

    def store(j):
        cols = pl.ds(pl.multiple_of(j * group * TW, TW), group * TW)
        return pltpu.make_async_copy(outv.at[:, cols], out_ref.at[:, cols], out_sem)

    @pl.loop(0, strips)
    def _(j):
        @pl.loop(0, group)
        def _(i):
            t = j * group + i
            col = pl.ds(pl.multiple_of(t * TW, TW), TW)
            for b in range(blocks):
                outv[blk(b), col] = inbox[sender[b], t]

        store(j).start()

    def sent_rows(way, rows):
        some = field.at[:, pl.ds(LAG + 1, tiles), rows]
        pltpu.make_async_copy(some, some, halo_send.at[way]).wait()

    @pl.when(has_up)
    def _():
        sent_rows(0, top)

    @pl.when(has_down)
    def _():
        sent_rows(1, bottom)

    all_of(outbox, sent, a2a_send)
    for way in range(2):
        on_sides(way, lambda copy: copy.wait_send())

    all_of(part_in, n_rows - 1, part_send)
    all_of(total_in, n_cols - 1, total_send)
    pltpu.make_async_copy(outv, outv, out_sem).wait()


def solution(mesh):
    n_rows, n_cols = mesh.shape["rows"], mesh.shape["cols"]

    def per_device(image, cloud_mask, tile_weight, owner):
        rows_here, width = image.shape
        blocks, tiles = rows_here // BR, width // TW
        strips = tiles // min(GROUP, tiles)
        pixel_total = float(owner.shape[0] * BR * width * n_cols)
        ext_rows, span = rows_here + 2 * BR, tiles + 2 * LAG
        small = (BR, TW)
        smem = pl.BlockSpec(memory_space=pltpu.SMEM)
        hbm = pl.BlockSpec(memory_space=pl.ANY)
        f32 = jnp.float32
        dma = pltpu.SemaphoreType.DMA
        out, obj = pl.pallas_call(
            functools.partial(kernel, n_rows, n_cols, pixel_total, ((1, n_rows),)),
            out_shape=(
                jax.ShapeDtypeStruct((rows_here, width), f32),
                jax.ShapeDtypeStruct((ITERS,), f32),
            ),
            in_specs=[smem, smem, hbm, hbm],
            out_specs=(hbm, smem),
            scratch_shapes=[
                pltpu.VMEM((2, span, ext_rows, TW), f32),
                pltpu.VMEM((span, rows_here, TW), f32),
                pltpu.VMEM((rows_here, width), jnp.int32),
            ]
            + [pltpu.VMEM((RING + 1, ext_rows, TW), f32)] * 16
            + [
                pltpu.VMEM((span, blocks, BR, TW), f32),
                pltpu.VMEM((n_rows, tiles, BR, TW), f32),
                pltpu.VMEM((n_rows, tiles, BR, TW), f32),
                pltpu.VMEM((rows_here, width), f32),
                pltpu.SMEM((n_rows,), jnp.int32),
                pltpu.SMEM((blocks,), jnp.int32),
                pltpu.VMEM(small, f32),
                pltpu.VMEM((n_rows,) + small, f32),
                pltpu.VMEM(small, f32),
                pltpu.VMEM((n_cols,) + small, f32),
                dma((strips,)),
                dma((strips,)),
                dma,
                dma((2,)),
                dma((2, strips)),
                dma((2, 3)),
                dma((2, 3)),
                dma,
                dma,
                dma,
                dma,
                dma,
                dma,
            ],
            compiler_params=pltpu.CompilerParams(
                collective_id=0, has_side_effects=True, vmem_limit_bytes=62 * 1024 * 1024
            ),
        )(tile_weight, owner, image, cloud_mask)
        return out, obj

    in_specs = (P("rows", "cols"), P("rows", "cols"), P("rows", "cols"), P())
    out_specs = (P("rows", "cols"), P())
    return jax.shard_map(
        per_device, mesh=mesh, in_specs=in_specs, out_specs=out_specs, check_vma=False
    )
```

```python
import functools

import jax
import jax.numpy as jnp
from jax import lax
from jax.experimental import pallas as pl
from jax.experimental.pallas import tpu as pltpu
from jax.sharding import PartitionSpec as P

MESH = pl.DeviceIdType.MESH
BR = 8
TW = 128
ITERS = 3
GROUP = 8
LAG = 16
RING = 8
OPTIONAL = 4
TINY = 1.2e-38

fidelity_scale = 0.25
tau_step = 0.35
sigma_step = 0.35
tv_weight = 0.3


def kernel(
    n_rows,
    n_cols,
    pixel_total,
    runs,
    weight_ref,
    owner_ref,
    image_ref,
    mask_ref,
    out_ref,
    obj_ref,
    field,
    fid,
    mask,
    pr0,
    pr1,
    pr2,
    pc0,
    pc1,
    pc2,
    er0,
    er1,
    er2,
    cr0,
    cr1,
    cr2,
    e0,
    e1,
    ex0,
    ex1,
    done,
    outbox,
    inbox,
    outv,
    pick,
    sender,
    part,
    part_in,
    total,
    total_in,
    load_sem,
    mask_sem,
    out_sem,
    halo_send,
    halo_recv,
    side_send,
    side_recv,
    a2a_send,
    a2a_recv,
    part_send,
    part_recv,
    total_send,
    total_recv,
):
    rows_here, width = image_ref.shape
    blocks = rows_here // BR
    tiles = width // TW
    group = min(GROUP, tiles)
    strips = tiles // group
    ext_blocks = blocks + 2
    ext_rows = rows_here + 2 * BR
    ext_tiles = tiles + 2
    me = lax.axis_index("rows")
    my_col = lax.axis_index("cols")
    has_up, has_down = me > 0, me < n_rows - 1
    has_left, has_right = my_col > 0, my_col < n_cols - 1
    own = pl.ds(BR, rows_here)

    def load_image(c, i):
        t = c * group + i
        return pltpu.make_async_copy(
            image_ref.at[:, pl.ds(pl.multiple_of(t * TW, TW), TW)],
            field.at[0, LAG + 1 + t, own],
            load_sem.at[c],
        )

    def load_mask(c):
        cols = pl.ds(pl.multiple_of(c * group * TW, TW), group * TW)
        return pltpu.make_async_copy(mask_ref.at[:, cols], mask.at[:, cols], mask_sem.at[c])

    @pl.loop(0, strips)
    def _(c):
        load_mask(c).start()

        @pl.loop(0, group)
        def _(i):
            load_image(c, i).start()

    barrier = pltpu.get_barrier_semaphore()

    @pl.loop(1, n_rows)
    def _(k):
        pl.semaphore_signal(
            barrier, inc=1, device_id={"rows": lax.rem(me + k, n_rows)}, device_id_type=MESH
        )

    @pl.loop(1, n_cols)
    def _(k):
        pl.semaphore_signal(
            barrier, inc=1, device_id={"cols": lax.rem(my_col + k, n_cols)}, device_id_type=MESH
        )

    up_row, down_row = lax.rem(me + n_rows - 1, n_rows), lax.rem(me + 1, n_rows)
    left_col, right_col = lax.rem(my_col + n_cols - 1, n_cols), lax.rem(my_col + 1, n_cols)
    for r in (up_row, down_row):
        for c in (left_col, right_col):
            pl.semaphore_signal(
                barrier, inc=1, device_id={"rows": r, "cols": c}, device_id_type=MESH
            )

    @pl.loop(0, n_rows)
    def _(d):
        found = jnp.int32(0)
        for b in range(blocks):
            found = jnp.where(owner_ref[me * blocks + b] == d, b, found)
        pick[d] = found

    def find_sender(s, carry):
        count, slots = carry
        mine = jnp.int32(0)
        for b in range(blocks):
            mine = jnp.where(owner_ref[s * blocks + b] == me, 1, mine)
        slots = [jnp.where((mine == 1) & (count == j), s, slots[j]) for j in range(blocks)]
        return count + mine, slots

    _, slots = lax.fori_loop(
        0, n_rows, find_sender, (jnp.int32(0), [jnp.int32(0)] * blocks)
    )
    for j in range(blocks):
        sender[j] = slots[j]

    @pl.loop(0, strips)
    def _(c):
        load_mask(c).wait()
        inner = field.at[0, pl.ds(LAG + 1 + c * group, group), own]
        pltpu.make_async_copy(inner, inner, load_sem.at[c]).wait()

        @pl.loop(0, group)
        def _(i):
            t = c * group + i
            col = pl.ds(pl.multiple_of(t * TW, TW), TW)
            for b in range(blocks):
                clear = (1 - mask[b * BR : (b + 1) * BR, col]).astype(jnp.float32)
                f = (fidelity_scale * weight_ref[b, t].astype(jnp.float32)) * clear
                fid[LAG + 1 + t, b * BR : (b + 1) * BR] = f
                field[1, LAG + 1 + t, (b + 1) * BR : (b + 2) * BR] = 1.0 / (1.0 + tau_step * f)

    zero = jnp.zeros((BR, TW), jnp.float32)
    slopes_r, slopes_c = (pr0, pr1, pr2), (pc0, pc1, pc2)
    rolled_e, rolled_c = (er0, er1, er2), (cr0, cr1, cr2)
    for pc in slopes_c:
        for b in range(ext_blocks):
            pc[RING, b * BR : (b + 1) * BR] = zero

    pl.semaphore_wait(barrier, n_rows - 1 + n_cols - 1 + 4)

    top, bottom = pl.ds(BR, BR), pl.ds(rows_here, BR)
    above, below_rows = pl.ds(0, BR), pl.ds(ext_rows - BR, BR)

    def halo(way, c):
        cols = pl.ds(LAG + 1 + c * group, group)
        src, dst = ((top, below_rows), (bottom, above))[way]
        return pltpu.make_async_remote_copy(
            src_ref=field.at[:, cols, src],
            dst_ref=field.at[:, cols, dst],
            send_sem=halo_send.at[way],
            recv_sem=halo_recv.at[way, c],
            device_id={"rows": (up_row, down_row)[way]},
            device_id_type=MESH,
        )

    def side(way, piece):
        src_col, dst_col = ((1, ext_tiles - 1), (ext_tiles - 2, 0))[way]
        src, dst = ((own, own), (top, below_rows), (bottom, above))[piece]
        device = {"cols": (left_col, right_col)[way]}
        if piece:
            device["rows"] = (up_row, down_row)[piece - 1]
        return pltpu.make_async_remote_copy(
            src_ref=field.at[:, pl.ds(LAG + src_col, 1), src],
            dst_ref=field.at[:, pl.ds(LAG + dst_col, 1), dst],
            send_sem=side_send.at[way, piece],
            recv_sem=side_recv.at[way, piece],
            device_id=device,
            device_id_type=MESH,
        )

    has_side, has_row = (has_left, has_right), (has_up, has_down)

    def on_sides(way, act):
        @pl.when(has_side[way])
        def _():
            act(side(way, 0))
            for piece in (1, 2):

                @pl.when(has_row[piece - 1])
                def _():
                    act(side(way, piece))

    def wait_side(way):
        @pl.when(has_side[1 - way])
        def _():
            side(way, 0).wait_recv()

            @pl.when(has_down)
            def _():
                side(way, 1).wait_recv()

            @pl.when(has_up)
            def _():
                side(way, 2).wait_recv()

    def on_rows(c, act_up, act_down):
        @pl.when(has_up)
        def _():
            act_up(c)

        @pl.when(has_down)
        def _():
            act_down(c)

    on_sides(1, lambda copy: copy.start())

    @pl.loop(0, strips)
    def _(c):
        on_rows(c, lambda c: halo(0, c).start(), lambda c: halo(1, c).start())

    on_sides(0, lambda copy: copy.start())

    def wait_halo(c):
        on_rows(c, lambda c: halo(1, c).wait_recv(), lambda c: halo(0, c).wait_recv())

    wait_side(1)

    sub = lax.broadcasted_iota(jnp.int32, (BR, TW), 0)
    lane = lax.broadcasted_iota(jnp.int32, (BR, TW), 1)
    first_lane, last_lane = lane == 0, lane == TW - 1
    end_row = jnp.logical_and(sub == BR - 1, jnp.logical_not(has_down))
    end_col = jnp.logical_and(last_lane, jnp.logical_not(has_right))
    reach = tv_weight / sigma_step
    gain_step = tau_step * sigma_step
    def blk(b):
        return slice(b * BR, (b + 1) * BR)

    def slot(at):
        return lax.rem(at + 2 * RING, RING)

    def ahead(step, at, rows):
        return field[0, LAG + at, rows] if step == 0 else (ex0, ex1)[step - 1][slot(at), rows]

    def inside(at, acc):
        return jnp.where(jnp.logical_and(at >= 1, at <= tiles), acc, 0.0)

    def roll_ahead(step, at):
        into = rolled_e[step]
        for b in range(ext_blocks if step < ITERS - 1 else ext_blocks - 1):
            e, after = ahead(step, at, blk(b)), ahead(step, at + 1, blk(b))
            into[slot(at), blk(b)] = pltpu.roll(jnp.where(first_lane, after, e), TW - 1, 1)

    def roll_slope(step, at):
        into, pc = rolled_c[step], slopes_c[step]
        edge = jnp.logical_and(at == 1, jnp.logical_not(has_left))
        before = jnp.where(edge, RING, slot(at - 1))
        for b in range(ext_blocks) if step < ITERS - 1 else range(1, blocks + 1):
            prior, here = pc[before, blk(b)], pc[slot(at), blk(b)]
            into[slot(at), blk(b)] = pltpu.roll(jnp.where(last_lane, prior, here), 1, 1)

    def dual(step, at):
        t = slot(at)
        stop_here = jnp.logical_and(end_col, at == tiles)
        pr, pc = slopes_r[step], slopes_c[step]
        acc = zero
        for b in range(ext_blocks if step < ITERS - 1 else ext_blocks - 1):
            e = ahead(step, at, blk(b))
            if b < ext_blocks - 1:
                below = ahead(step, at, slice(b * BR + 1, (b + 1) * BR + 1))
            else:
                below = pltpu.roll(e, BR - 1, 0)
            g_r = below - e
            if b == blocks:
                g_r = jnp.where(end_row, 0.0, g_r)
            g_c = jnp.where(stop_here, 0.0, rolled_e[step][t, blk(b)] - e)
            mine = 0 < b <= blocks
            if step == 0:
                q_r, q_c = g_r, g_c
                q2 = q_r * q_r + q_c * q_c
                inv_len = lax.rsqrt(jnp.maximum(q2, TINY))
                if mine:
                    acc = acc + q2 * inv_len
            else:
                q_r = g_r + slopes_r[step - 1][t, blk(b)]
                q_c = g_c + slopes_c[step - 1][t, blk(b)]
                inv_len = lax.rsqrt(q_r * q_r + q_c * q_c)
                if mine:
                    g2 = g_r * g_r + g_c * g_c
                    acc = acc + g2 * lax.rsqrt(jnp.maximum(g2, TINY))
            inv = jnp.minimum(1.0, reach * inv_len)
            p_r = q_r * inv
            if b == 0:
                p_r = jnp.where(has_up, p_r, 0.0)
            pr[t, blk(b)] = p_r
            pc[t, blk(b)] = q_c * inv
        return inside(at, acc)

    def primal(step, at):
        t, full = slot(at), LAG + at
        pr, pc = slopes_r[step], slopes_c[step]
        acc = zero
        for b in range(ext_blocks) if step < ITERS - 1 else range(1, blocks + 1):
            p_r, p_c = pr[t, blk(b)], pc[t, blk(b)]
            if b > 0:
                over = pr[t, b * BR - 1 : (b + 1) * BR - 1]
            else:
                over = pltpu.roll(p_r, 1, 0)
            div = gain_step * ((p_r - over) + (p_c - rolled_c[step][t, blk(b)]))
            observed, g = field[0, full, blk(b)], field[1, full, blk(b)]
            if step == 0:
                e = div * g
                e0[t, blk(b)] = e
                ex0[t, blk(b)] = observed + 2.0 * e
            elif step == 1:
                old = e0[t, blk(b)]
                e = (old + div) * g
                e1[t, blk(b)] = e
                ex1[t, blk(b)] = (observed - old) + 2.0 * e
            else:
                e = (e1[t, blk(b)] + div) * g
                done[full, b - 1] = observed + e
            if 0 < b <= blocks:
                acc = acc + fid[full, blk(b - 1)] * (e * e)
        return inside(at, acc)

    def sweep(t, sums):
        sums = list(sums)
        for step in reversed(range(ITERS)):
            at = t - 5 * step
            sums[2 * step] += primal(step, at - 3)
            roll_slope(step, at - 2)
            sums[2 * step + 1] += dual(step, at - 1)
            roll_ahead(step, at)
        return tuple(sums)

    def block_copy(k, j):
        target = lax.rem(me + k, n_rows)
        part_of = pl.ds(j * group, group)
        return pltpu.make_async_remote_copy(
            src_ref=outbox.at[target, part_of],
            dst_ref=inbox.at[me, part_of],
            send_sem=a2a_send,
            recv_sem=a2a_recv,
            device_id={"rows": target},
            device_id_type=MESH,
        )

    def strip(j, sums):
        @pl.when(j < strips)
        def _():
            wait_halo(j)

        @pl.when(j == strips)
        def _():
            wait_side(0)

        sums = lax.fori_loop(0, group, lambda i, s: sweep(j * group + i - 2, s), sums)

        @pl.when(j > 1)
        def _():
            here = pl.ds((j - 2) * group, group)
            ext_here = pl.ds(LAG + 1 + (j - 2) * group, group)
            for first, stop in runs:

                @pl.loop(first, stop)
                def _(k):
                    target = lax.rem(me + k, n_rows)
                    outbox[target, here] = done[ext_here, pick[target]]
                    block_copy(k, j - 2).start()

            inbox[me, here] = done[ext_here, pick[me]]

        return sums

    sums = lax.fori_loop(0, strips + 2, strip, (zero,) * (2 * ITERS))

    stacked = zero
    for step in range(ITERS):
        acc = 0.5 * sums[2 * step] + tv_weight * sums[2 * step + 1]
        one = jnp.sum(jnp.sum(acc, axis=1, keepdims=True), axis=0, keepdims=True)
        stacked = jnp.where(sub == step, one, stacked)
    part[...] = stacked

    def part_copy(k):
        return pltpu.make_async_remote_copy(
            src_ref=part,
            dst_ref=part_in.at[me],
            send_sem=part_send,
            recv_sem=part_recv,
            device_id={"rows": lax.rem(me + k, n_rows)},
            device_id_type=MESH,
        )

    def all_of(buffer, count, sem):
        some = buffer.at[pl.ds(0, count)]
        pltpu.make_async_copy(some, some, sem).wait()

    @pl.loop(1, n_rows)
    def _(k):
        part_copy(k).start()

    part_in[me] = stacked

    all_of(part_in, n_rows - 1, part_recv)

    total_here = lax.fori_loop(0, n_rows, lambda k, s: s + part_in[k], zero)
    total[...] = total_here
    total_in[my_col] = total_here

    def total_copy(k):
        return pltpu.make_async_remote_copy(
            src_ref=total,
            dst_ref=total_in.at[my_col],
            send_sem=total_send,
            recv_sem=total_recv,
            device_id={"cols": lax.rem(my_col + k, n_cols)},
            device_id_type=MESH,
        )

    @pl.loop(1, n_cols)
    def _(k):
        total_copy(k).start()

    all_of(total_in, n_cols - 1, total_recv)

    everything = lax.fori_loop(0, n_cols, lambda k, s: s + total_in[k], zero)
    everything = everything / pixel_total
    for step in range(ITERS):
        obj_ref[step] = everything[step, 0]

    sent = sum(stop - first for first, stop in runs)
    all_of(inbox, sent, a2a_recv)

    def store(j):
        cols = pl.ds(pl.multiple_of(j * group * TW, TW), group * TW)
        return pltpu.make_async_copy(outv.at[:, cols], out_ref.at[:, cols], out_sem)

    @pl.loop(0, strips)
    def _(j):
        @pl.loop(0, group)
        def _(i):
            t = j * group + i
            col = pl.ds(pl.multiple_of(t * TW, TW), TW)
            for b in range(blocks):
                outv[blk(b), col] = inbox[sender[b], t]

        store(j).start()

    def sent_rows(way, rows):
        some = field.at[:, pl.ds(LAG + 1, tiles), rows]
        pltpu.make_async_copy(some, some, halo_send.at[way]).wait()

    @pl.when(has_up)
    def _():
        sent_rows(0, top)

    @pl.when(has_down)
    def _():
        sent_rows(1, bottom)

    all_of(outbox, sent, a2a_send)
    for way in range(2):
        on_sides(way, lambda copy: copy.wait_send())

    all_of(part_in, n_rows - 1, part_send)
    all_of(total_in, n_cols - 1, total_send)
    pltpu.make_async_copy(outv, outv, out_sem).wait()


def spans(numbers):
    found = []
    for number in sorted(numbers):
        if found and found[-1][1] == number:
            found[-1][1] = number + 1
        else:
            found.append([number, number + 1])
    return tuple(map(tuple, found))


def solution(mesh):
    n_rows, n_cols = mesh.shape["rows"], mesh.shape["cols"]

    def per_device(image, cloud_mask, tile_weight, owner):
        rows_here, width = image.shape
        blocks, tiles = rows_here // BR, width // TW
        strips = tiles // min(GROUP, tiles)
        pixel_total = float(owner.shape[0] * BR * width * n_cols)
        ext_rows, span = rows_here + 2 * BR, tiles + 2 * LAG
        small = (BR, TW)
        smem = pl.BlockSpec(memory_space=pltpu.SMEM)
        hbm = pl.BlockSpec(memory_space=pl.ANY)
        f32 = jnp.float32
        dma = pltpu.SemaphoreType.DMA

        dear = [k for i in range(1, OPTIONAL // 2 + 1) for k in (n_rows // 2 - i, n_rows // 2 + i)]
        home = jnp.arange(owner.shape[0], dtype=jnp.int32) // blocks
        turn = lax.rem(owner - home + n_rows, n_rows)
        bits = jnp.zeros_like(turn)
        for i, k in enumerate(dear):
            bits = bits | jnp.where(turn == k, 1 << i, 0)
        which = lax.reduce(bits, jnp.int32(0), lax.bitwise_or, (0,))

        def variant(number):
            left_out = [k for i, k in enumerate(dear) if not number >> i & 1]
            runs = spans(set(range(1, n_rows)) - set(left_out))
            return functools.partial(call, number, runs)

        def call(number, runs, *operands):
            return pl.pallas_call(
                functools.partial(kernel, n_rows, n_cols, pixel_total, runs),
                out_shape=(
                    jax.ShapeDtypeStruct((rows_here, width), f32),
                    jax.ShapeDtypeStruct((ITERS,), f32),
                ),
                in_specs=[smem, smem, hbm, hbm],
                out_specs=(hbm, smem),
                scratch_shapes=[
                    pltpu.VMEM((2, span, ext_rows, TW), f32),
                    pltpu.VMEM((span, rows_here, TW), f32),
                    pltpu.VMEM((rows_here, width), jnp.int32),
                ]
                + [pltpu.VMEM((RING + 1, ext_rows, TW), f32)] * 16
                + [
                    pltpu.VMEM((span, blocks, BR, TW), f32),
                    pltpu.VMEM((n_rows, tiles, BR, TW), f32),
                    pltpu.VMEM((n_rows, tiles, BR, TW), f32),
                    pltpu.VMEM((rows_here, width), f32),
                    pltpu.SMEM((n_rows,), jnp.int32),
                    pltpu.SMEM((blocks,), jnp.int32),
                    pltpu.VMEM(small, f32),
                    pltpu.VMEM((n_rows,) + small, f32),
                    pltpu.VMEM(small, f32),
                    pltpu.VMEM((n_cols,) + small, f32),
                    dma((strips,)),
                    dma((strips,)),
                    dma,
                    dma((2,)),
                    dma((2, strips)),
                    dma((2, 3)),
                    dma((2, 3)),
                    dma,
                    dma,
                    dma,
                    dma,
                    dma,
                    dma,
                ],
                compiler_params=pltpu.CompilerParams(
                    collective_id=number, has_side_effects=True, vmem_limit_bytes=62 * 1024 * 1024
                ),
            )(*operands)

        variants = [variant(number) for number in range(1 << OPTIONAL)]
        return lax.switch(which, variants, tile_weight, owner, image, cloud_mask)

    in_specs = (P("rows", "cols"), P("rows", "cols"), P("rows", "cols"), P())
    out_specs = (P("rows", "cols"), P())
    return jax.shard_map(
        per_device, mesh=mesh, in_specs=in_specs, out_specs=out_specs, check_vma=False
    )
```

```python
import functools

import jax
import jax.numpy as jnp
from jax import lax
from jax.experimental import pallas as pl
from jax.experimental.pallas import tpu as pltpu
from jax.sharding import PartitionSpec as P

MESH = pl.DeviceIdType.MESH
BR = 8
TW = 128
ITERS = 3
GROUP = 8
LAG = 16
RING = 8
OPTIONAL = 5
TINY = 1.2e-38

fidelity_scale = 0.25
tau_step = 0.35
sigma_step = 0.35
tv_weight = 0.3


def kernel(
    n_rows,
    n_cols,
    pixel_total,
    runs,
    weight_ref,
    owner_ref,
    image_ref,
    mask_ref,
    out_ref,
    obj_ref,
    field,
    fid,
    mask,
    pr0,
    pr1,
    pr2,
    pc0,
    pc1,
    pc2,
    er0,
    er1,
    er2,
    cr0,
    cr1,
    cr2,
    e0,
    e1,
    ex0,
    ex1,
    done,
    outbox,
    inbox,
    inbox_last,
    outv,
    pick,
    sender,
    part,
    part_in,
    total,
    total_in,
    load_sem,
    mask_sem,
    out_sem,
    halo_send,
    halo_recv,
    side_send,
    side_recv,
    a2a_send,
    a2a_recv,
    last_recv,
    part_send,
    part_recv,
    total_send,
    total_recv,
):
    rows_here, width = image_ref.shape
    blocks = rows_here // BR
    tiles = width // TW
    group = min(GROUP, tiles)
    strips = tiles // group
    ext_blocks = blocks + 2
    ext_rows = rows_here + 2 * BR
    ext_tiles = tiles + 2
    me = lax.axis_index("rows")
    my_col = lax.axis_index("cols")
    has_up, has_down = me > 0, me < n_rows - 1
    has_left, has_right = my_col > 0, my_col < n_cols - 1
    own = pl.ds(BR, rows_here)

    def load_image(c, i):
        t = c * group + i
        return pltpu.make_async_copy(
            image_ref.at[:, pl.ds(pl.multiple_of(t * TW, TW), TW)],
            field.at[0, LAG + 1 + t, own],
            load_sem.at[c],
        )

    def load_mask(c):
        cols = pl.ds(pl.multiple_of(c * group * TW, TW), group * TW)
        return pltpu.make_async_copy(mask_ref.at[:, cols], mask.at[:, cols], mask_sem.at[c])

    barrier = pltpu.get_barrier_semaphore()

    @pl.loop(1, n_rows)
    def _(k):
        pl.semaphore_signal(
            barrier, inc=1, device_id={"rows": lax.rem(me + k, n_rows)}, device_id_type=MESH
        )

    @pl.loop(1, n_cols)
    def _(k):
        pl.semaphore_signal(
            barrier, inc=1, device_id={"cols": lax.rem(my_col + k, n_cols)}, device_id_type=MESH
        )

    up_row, down_row = lax.rem(me + n_rows - 1, n_rows), lax.rem(me + 1, n_rows)
    left_col, right_col = lax.rem(my_col + n_cols - 1, n_cols), lax.rem(my_col + 1, n_cols)
    for r in (up_row, down_row):
        for c in (left_col, right_col):
            pl.semaphore_signal(
                barrier, inc=1, device_id={"rows": r, "cols": c}, device_id_type=MESH
            )

    def turn(c):
        return lax.rem(c + strips - 1, strips)

    @pl.loop(0, strips)
    def _(n):
        c = turn(n)
        load_mask(c).start()

        @pl.loop(0, group)
        def _(i):
            load_image(c, i).start()

    def prepare(c):
        load_mask(c).wait()
        inner = field.at[0, pl.ds(LAG + 1 + c * group, group), own]
        pltpu.make_async_copy(inner, inner, load_sem.at[c]).wait()

        @pl.loop(0, group)
        def _(i):
            t = c * group + i
            col = pl.ds(pl.multiple_of(t * TW, TW), TW)
            for b in range(blocks):
                clear = (1 - mask[b * BR : (b + 1) * BR, col]).astype(jnp.float32)
                f = (fidelity_scale * weight_ref[b, t].astype(jnp.float32)) * clear
                fid[LAG + 1 + t, b * BR : (b + 1) * BR] = f
                field[1, LAG + 1 + t, (b + 1) * BR : (b + 2) * BR] = 1.0 / (1.0 + tau_step * f)

    zero = jnp.zeros((BR, TW), jnp.float32)
    slopes_r, slopes_c = (pr0, pr1, pr2), (pc0, pc1, pc2)
    rolled_e, rolled_c = (er0, er1, er2), (cr0, cr1, cr2)
    for pc in slopes_c:
        for b in range(ext_blocks):
            pc[RING, b * BR : (b + 1) * BR] = zero

    outer = min(2, strips)

    @pl.loop(0, outer)
    def _(n):
        prepare(turn(n))

    pl.semaphore_wait(barrier, n_rows - 1 + n_cols - 1 + 4)

    top, bottom = pl.ds(BR, BR), pl.ds(rows_here, BR)
    above, below_rows = pl.ds(0, BR), pl.ds(ext_rows - BR, BR)

    def halo(way, c):
        cols = pl.ds(LAG + 1 + c * group, group)
        src, dst = ((top, below_rows), (bottom, above))[way]
        return pltpu.make_async_remote_copy(
            src_ref=field.at[:, cols, src],
            dst_ref=field.at[:, cols, dst],
            send_sem=halo_send.at[way],
            recv_sem=halo_recv.at[way, c],
            device_id={"rows": (up_row, down_row)[way]},
            device_id_type=MESH,
        )

    def side(way, piece):
        src_col, dst_col = ((1, ext_tiles - 1), (ext_tiles - 2, 0))[way]
        src, dst = ((own, own), (top, below_rows), (bottom, above))[piece]
        device = {"cols": (left_col, right_col)[way]}
        if piece:
            device["rows"] = (up_row, down_row)[piece - 1]
        return pltpu.make_async_remote_copy(
            src_ref=field.at[:, pl.ds(LAG + src_col, 1), src],
            dst_ref=field.at[:, pl.ds(LAG + dst_col, 1), dst],
            send_sem=side_send.at[way, piece],
            recv_sem=side_recv.at[way, piece],
            device_id=device,
            device_id_type=MESH,
        )

    has_side, has_row = (has_left, has_right), (has_up, has_down)

    def on_sides(way, act):
        @pl.when(has_side[way])
        def _():
            act(side(way, 0))
            for piece in (1, 2):

                @pl.when(has_row[piece - 1])
                def _():
                    act(side(way, piece))

    def wait_side(way):
        @pl.when(has_side[1 - way])
        def _():
            side(way, 0).wait_recv()

            @pl.when(has_down)
            def _():
                side(way, 1).wait_recv()

            @pl.when(has_up)
            def _():
                side(way, 2).wait_recv()

    def on_rows(c, act_up, act_down):
        @pl.when(has_up)
        def _():
            act_up(c)

        @pl.when(has_down)
        def _():
            act_down(c)

    def start_halo(c):
        on_rows(c, lambda c: halo(0, c).start(), lambda c: halo(1, c).start())

    on_sides(1, lambda copy: copy.start())

    @pl.loop(1, outer + 1)
    def _(n):
        start_halo(turn(lax.rem(n, outer)))

    on_sides(0, lambda copy: copy.start())

    @pl.loop(outer, strips)
    def _(n):
        c = turn(n)
        prepare(c)
        start_halo(c)

    @pl.loop(0, n_rows)
    def _(d):
        found = jnp.int32(0)
        for b in range(blocks):
            found = jnp.where(owner_ref[me * blocks + b] == d, b, found)
        pick[d] = found

    def find_sender(s, carry):
        count, slots = carry
        mine = jnp.int32(0)
        for b in range(blocks):
            mine = jnp.where(owner_ref[s * blocks + b] == me, 1, mine)
        slots = [jnp.where((mine == 1) & (count == j), s, slots[j]) for j in range(blocks)]
        return count + mine, slots

    _, slots = lax.fori_loop(
        0, n_rows, find_sender, (jnp.int32(0), [jnp.int32(0)] * blocks)
    )
    for j in range(blocks):
        sender[j] = slots[j]

    def wait_halo(c):
        on_rows(c, lambda c: halo(1, c).wait_recv(), lambda c: halo(0, c).wait_recv())

    wait_side(1)

    sub = lax.broadcasted_iota(jnp.int32, (BR, TW), 0)
    lane = lax.broadcasted_iota(jnp.int32, (BR, TW), 1)
    first_lane, last_lane = lane == 0, lane == TW - 1
    end_row = jnp.logical_and(sub == BR - 1, jnp.logical_not(has_down))
    end_col = jnp.logical_and(last_lane, jnp.logical_not(has_right))
    reach = tv_weight / sigma_step
    gain_step = tau_step * sigma_step
    def blk(b):
        return slice(b * BR, (b + 1) * BR)

    def slot(at):
        return lax.rem(at + 2 * RING, RING)

    def ahead(step, at, rows):
        return field[0, LAG + at, rows] if step == 0 else (ex0, ex1)[step - 1][slot(at), rows]

    def inside(at, acc):
        return jnp.where(jnp.logical_and(at >= 1, at <= tiles), acc, 0.0)

    def roll_ahead(step, at):
        into = rolled_e[step]
        for b in range(ext_blocks if step < ITERS - 1 else ext_blocks - 1):
            e, after = ahead(step, at, blk(b)), ahead(step, at + 1, blk(b))
            into[slot(at), blk(b)] = pltpu.roll(jnp.where(first_lane, after, e), TW - 1, 1)

    def roll_slope(step, at):
        into, pc = rolled_c[step], slopes_c[step]
        edge = jnp.logical_and(at == 1, jnp.logical_not(has_left))
        before = jnp.where(edge, RING, slot(at - 1))
        for b in range(ext_blocks) if step < ITERS - 1 else range(1, blocks + 1):
            prior, here = pc[before, blk(b)], pc[slot(at), blk(b)]
            into[slot(at), blk(b)] = pltpu.roll(jnp.where(last_lane, prior, here), 1, 1)

    def dual(step, at):
        t = slot(at)
        stop_here = jnp.logical_and(end_col, at == tiles)
        pr, pc = slopes_r[step], slopes_c[step]
        acc = zero
        for b in range(ext_blocks if step < ITERS - 1 else ext_blocks - 1):
            e = ahead(step, at, blk(b))
            if b < ext_blocks - 1:
                below = ahead(step, at, slice(b * BR + 1, (b + 1) * BR + 1))
            else:
                below = pltpu.roll(e, BR - 1, 0)
            g_r = below - e
            if b == blocks:
                g_r = jnp.where(end_row, 0.0, g_r)
            g_c = jnp.where(stop_here, 0.0, rolled_e[step][t, blk(b)] - e)
            mine = 0 < b <= blocks
            if step == 0:
                q_r, q_c = g_r, g_c
                q2 = q_r * q_r + q_c * q_c
                inv_len = lax.rsqrt(jnp.maximum(q2, TINY))
                if mine:
                    acc = acc + q2 * inv_len
            else:
                q_r = g_r + slopes_r[step - 1][t, blk(b)]
                q_c = g_c + slopes_c[step - 1][t, blk(b)]
                inv_len = lax.rsqrt(q_r * q_r + q_c * q_c)
                if mine:
                    g2 = g_r * g_r + g_c * g_c
                    acc = acc + g2 * lax.rsqrt(jnp.maximum(g2, TINY))
            inv = jnp.minimum(1.0, reach * inv_len)
            p_r = q_r * inv
            if b == 0:
                p_r = jnp.where(has_up, p_r, 0.0)
            pr[t, blk(b)] = p_r
            pc[t, blk(b)] = q_c * inv
        return inside(at, acc)

    def primal(step, at):
        t, full = slot(at), LAG + at
        pr, pc = slopes_r[step], slopes_c[step]
        acc = zero
        for b in range(ext_blocks) if step < ITERS - 1 else range(1, blocks + 1):
            p_r, p_c = pr[t, blk(b)], pc[t, blk(b)]
            if b > 0:
                over = pr[t, b * BR - 1 : (b + 1) * BR - 1]
            else:
                over = pltpu.roll(p_r, 1, 0)
            div = gain_step * ((p_r - over) + (p_c - rolled_c[step][t, blk(b)]))
            observed, g = field[0, full, blk(b)], field[1, full, blk(b)]
            if step == 0:
                e = div * g
                e0[t, blk(b)] = e
                ex0[t, blk(b)] = observed + 2.0 * e
            elif step == 1:
                old = e0[t, blk(b)]
                e = (old + div) * g
                e1[t, blk(b)] = e
                ex1[t, blk(b)] = (observed - old) + 2.0 * e
            else:
                e = (e1[t, blk(b)] + div) * g
                done[full, b - 1] = observed + e
            if 0 < b <= blocks:
                acc = acc + fid[full, blk(b - 1)] * (e * e)
        return inside(at, acc)

    def sweep(t, sums):
        sums = list(sums)
        for step in reversed(range(ITERS)):
            at = t - 5 * step
            sums[2 * step] += primal(step, at - 3)
            roll_slope(step, at - 2)
            sums[2 * step + 1] += dual(step, at - 1)
            roll_ahead(step, at)
        return tuple(sums)

    early = strips - 1

    def block_copy(k, j, last):
        target = lax.rem(me + k, n_rows)
        part_of = pl.ds(j * group, group)
        return pltpu.make_async_remote_copy(
            src_ref=outbox.at[target, part_of],
            dst_ref=inbox_last.at[me] if last else inbox.at[me, part_of],
            send_sem=a2a_send,
            recv_sem=last_recv if last else a2a_recv,
            device_id={"rows": target},
            device_id_type=MESH,
        )

    def strip(j, sums):
        @pl.when(j < strips)
        def _():
            wait_halo(j)

        @pl.when(j == strips)
        def _():
            wait_side(0)

        sums = lax.fori_loop(0, group, lambda i, s: sweep(j * group + i - 2, s), sums)

        def send(j, last):
            here = pl.ds(j * group, group)
            ext_here = pl.ds(LAG + 1 + j * group, group)
            for first, stop in runs:

                @pl.loop(first, stop)
                def _(k):
                    target = lax.rem(me + k, n_rows)
                    outbox[target, here] = done[ext_here, pick[target]]
                    block_copy(k, j, last).start()

            if last:
                inbox_last[me] = done[ext_here, pick[me]]
            else:
                inbox[me, here] = done[ext_here, pick[me]]

        @pl.when(jnp.logical_and(j > 1, j < strips + 1))
        def _():
            send(j - 2, False)

        @pl.when(j == strips + 1)
        def _():
            send(j - 2, True)

        return sums

    sums = lax.fori_loop(0, strips + 2, strip, (zero,) * (2 * ITERS))

    stacked = zero
    for step in range(ITERS):
        acc = 0.5 * sums[2 * step] + tv_weight * sums[2 * step + 1]
        one = jnp.sum(jnp.sum(acc, axis=1, keepdims=True), axis=0, keepdims=True)
        stacked = jnp.where(sub == step, one, stacked)
    part[...] = stacked

    def part_copy(k):
        return pltpu.make_async_remote_copy(
            src_ref=part,
            dst_ref=part_in.at[me],
            send_sem=part_send,
            recv_sem=part_recv,
            device_id={"rows": lax.rem(me + k, n_rows)},
            device_id_type=MESH,
        )

    def all_of(buffer, count, sem):
        some = buffer.at[pl.ds(0, count)]
        pltpu.make_async_copy(some, some, sem).wait()

    @pl.loop(1, n_rows)
    def _(k):
        part_copy(k).start()

    part_in[me] = stacked

    all_of(part_in, n_rows - 1, part_recv)

    total_here = lax.fori_loop(0, n_rows, lambda k, s: s + part_in[k], zero)
    total[...] = total_here
    total_in[my_col] = total_here

    def total_copy(k):
        return pltpu.make_async_remote_copy(
            src_ref=total,
            dst_ref=total_in.at[my_col],
            send_sem=total_send,
            recv_sem=total_recv,
            device_id={"cols": lax.rem(my_col + k, n_cols)},
            device_id_type=MESH,
        )

    @pl.loop(1, n_cols)
    def _(k):
        total_copy(k).start()

    all_of(total_in, n_cols - 1, total_recv)

    everything = lax.fori_loop(0, n_cols, lambda k, s: s + total_in[k], zero)
    everything = everything / pixel_total
    for step in range(ITERS):
        obj_ref[step] = everything[step, 0]

    sent = sum(stop - first for first, stop in runs)
    def store(j):
        cols = pl.ds(pl.multiple_of(j * group * TW, TW), group * TW)
        return pltpu.make_async_copy(outv.at[:, cols], out_ref.at[:, cols], out_sem)

    def put(j, last):
        @pl.loop(0, group)
        def _(i):
            t = j * group + i
            col = pl.ds(pl.multiple_of(t * TW, TW), TW)
            for b in range(blocks):
                outv[blk(b), col] = inbox_last[sender[b], i] if last else inbox[sender[b], t]

        store(j).start()

    if early:
        arrived = inbox.at[pl.ds(0, sent), pl.ds(0, early * group)]
        pltpu.make_async_copy(arrived, arrived, a2a_recv).wait()

        @pl.loop(0, early)
        def _(j):
            put(j, False)

    all_of(inbox_last, sent, last_recv)
    put(early, True)

    def sent_rows(way, rows):
        some = field.at[:, pl.ds(LAG + 1, tiles), rows]
        pltpu.make_async_copy(some, some, halo_send.at[way]).wait()

    @pl.when(has_up)
    def _():
        sent_rows(0, top)

    @pl.when(has_down)
    def _():
        sent_rows(1, bottom)

    all_of(outbox, sent, a2a_send)
    for way in range(2):
        on_sides(way, lambda copy: copy.wait_send())

    all_of(part_in, n_rows - 1, part_send)
    all_of(total_in, n_cols - 1, total_send)
    pltpu.make_async_copy(outv, outv, out_sem).wait()


def spans(numbers):
    found = []
    for number in sorted(numbers):
        if found and found[-1][1] == number:
            found[-1][1] = number + 1
        else:
            found.append([number, number + 1])
    return tuple(map(tuple, found))


def solution(mesh):
    n_rows, n_cols = mesh.shape["rows"], mesh.shape["cols"]

    def per_device(image, cloud_mask, tile_weight, owner):
        rows_here, width = image.shape
        blocks, tiles = rows_here // BR, width // TW
        strips = tiles // min(GROUP, tiles)
        pixel_total = float(owner.shape[0] * BR * width * n_cols)
        ext_rows, span = rows_here + 2 * BR, tiles + 2 * LAG
        small = (BR, TW)
        smem = pl.BlockSpec(memory_space=pltpu.SMEM)
        hbm = pl.BlockSpec(memory_space=pl.ANY)
        f32 = jnp.float32
        dma = pltpu.SemaphoreType.DMA

        pairs = [(n_rows // 2 - i, n_rows // 2 + i) for i in range(1, (OPTIONAL + 3) // 2)]
        dear = [k for pair in pairs for k in pair][:OPTIONAL]
        home = jnp.arange(owner.shape[0], dtype=jnp.int32) // blocks
        turn = lax.rem(owner - home + n_rows, n_rows)
        bits = jnp.zeros_like(turn)
        for i, k in enumerate(dear):
            bits = bits | jnp.where(turn == k, 1 << i, 0)
        which = lax.reduce(bits, jnp.int32(0), lax.bitwise_or, (0,))

        def variant(number):
            left_out = [k for i, k in enumerate(dear) if not number >> i & 1]
            runs = spans(set(range(1, n_rows)) - set(left_out))
            return functools.partial(call, number, runs)

        def call(number, runs, *operands):
            return pl.pallas_call(
                functools.partial(kernel, n_rows, n_cols, pixel_total, runs),
                out_shape=(
                    jax.ShapeDtypeStruct((rows_here, width), f32),
                    jax.ShapeDtypeStruct((ITERS,), f32),
                ),
                in_specs=[smem, smem, hbm, hbm],
                out_specs=(hbm, smem),
                scratch_shapes=[
                    pltpu.VMEM((2, span, ext_rows, TW), f32),
                    pltpu.VMEM((span, rows_here, TW), f32),
                    pltpu.VMEM((rows_here, width), jnp.int32),
                ]
                + [pltpu.VMEM((RING + 1, ext_rows, TW), f32)] * 16
                + [
                    pltpu.VMEM((span, blocks, BR, TW), f32),
                    pltpu.VMEM((n_rows, tiles, BR, TW), f32),
                    pltpu.VMEM((n_rows, tiles, BR, TW), f32),
                    pltpu.VMEM((n_rows, tiles // strips, BR, TW), f32),
                    pltpu.VMEM((rows_here, width), f32),
                    pltpu.SMEM((n_rows,), jnp.int32),
                    pltpu.SMEM((blocks,), jnp.int32),
                    pltpu.VMEM(small, f32),
                    pltpu.VMEM((n_rows,) + small, f32),
                    pltpu.VMEM(small, f32),
                    pltpu.VMEM((n_cols,) + small, f32),
                    dma((strips,)),
                    dma((strips,)),
                    dma,
                    dma((2,)),
                    dma((2, strips)),
                    dma((2, 3)),
                    dma((2, 3)),
                    dma,
                    dma,
                    dma,
                    dma,
                    dma,
                    dma,
                    dma,
                ],
                compiler_params=pltpu.CompilerParams(
                    collective_id=number, has_side_effects=True, vmem_limit_bytes=62 * 1024 * 1024
                ),
            )(*operands)

        variants = [variant(number) for number in range(1 << OPTIONAL)]
        return lax.switch(which, variants, tile_weight, owner, image, cloud_mask)

    in_specs = (P("rows", "cols"), P("rows", "cols"), P("rows", "cols"), P())
    out_specs = (P("rows", "cols"), P())
    return jax.shard_map(
        per_device, mesh=mesh, in_specs=in_specs, out_specs=out_specs, check_vma=False
    )
```
